32 devices in a mesh: dp: 16 (over z, y, core), space: 2 (over x).
Axes of the slice: x: 2, y: 2, z: 4, core: 2. Of those that a mesh axis runs over, the one named last changes fastest.
Arguments:
- images: bfloat16 [16, 3, 512, 512], P('dp', None, 'space'), may hold values from -6 to 6
- pos_embed: bfloat16 [1024, 1280], P('space'), may hold values from -3 to 3
- conv_first: bfloat16 [3, 3, 3, 64], replicated, may hold values from -1.75 to 1.75
- conv_second: bfloat16 [3, 3, 64, 128], replicated, may hold values from -0.375 to 0.375
- conv_third: bfloat16 [3, 3, 128, 256], replicated, may hold values from -0.25 to 0.25
- conv_fourth: bfloat16 [3, 3, 256, 512], replicated, may hold values from -0.1875 to 0.1875
- proj_weight: bfloat16 [512, 1280], replicated, may hold values from -0.375 to 0.375
- ln_first: float32 [1280], replicated, may hold values from 0.25 to 1.75
- qkv_weight: bfloat16 [1280, 3, 1280], P('dp', None, 'space'), as said below
- out_weight: bfloat16 [1280, 1280], P('space', 'dp'), may hold values from -0.15625 to 0.15625
- ln_second: float32 [1280], replicated, may hold values from 0.25 to 1.75
- up_weight: bfloat16 [1280, 5120], P('dp', 'space'), may hold values from -0.15625 to 0.15625
- down_weight: bfloat16 [5120, 1280], P('space', 'dp'), may hold values from -0.125 to 0.125
Outputs:
- encoded: bfloat16 [16, 1024, 1280], P('dp', 'space')
The draws below stay inside these ranges and needn't reach their ends.
Inputs may be any that keep to these rules, and one draw needn't show every extreme that they name: `qkv_weight`: every entry is at most 135 * 1280 ** -0.5 in magnitude.
All inputs are finite; a program needn't handle non-finite values.
Results may differ from the reference program's by a relative error of at most 0.014.
Values may be sent and summed in bfloat16 or wider, within the bound.
A program may use at most 128 MiB of HBM per device.

```python
import jax
import jax.numpy as jnp
from jax import lax

D = 1280
HEADS = 16
FF = 5120
C1 = 64
C2 = 128
C3 = 256
C4 = 512
RES = 512
TOKS = 1024
IMAGES = 16
N_SPACE = 2


def draw_qkv_weight(key, part):
    first = jax.random.fold_in(jax.random.fold_in(key, 7), 0)
    base = jnp.clip(jax.random.normal(first, (D, 3, D), jnp.float32), -4.5, 4.5) / jnp.sqrt(jnp.float32(D))
    return base.astype(jnp.bfloat16)


def block_levels(own_key, shape, cuts, smallest, high):
    level, own = 1.0, jax.random.fold_in(own_key, 6)
    for position, blocks in cuts:
        draws = jnp.exp(jax.random.uniform(jax.random.fold_in(own, position), (blocks,), jnp.float32, smallest / len(cuts), high / len(cuts)))
        level = level * jnp.repeat(draws, shape[position] // blocks).reshape([-1 if axis == position else 1 for axis in range(len(shape))])
    return level


def bell_draw(rng, shape, scale, reach, pieces=(), dtype=jnp.bfloat16):
    level = block_levels(rng, shape, pieces, -0.22, 0.18) if pieces else 1.0
    entries = jax.random.normal(rng, shape, jnp.float32) * scale * level
    return jnp.minimum(jnp.maximum(entries, -reach), reach).astype(dtype)


def setup_inputs(seed: int = 0) -> dict:
    splits = jax.random.split(jax.random.key(seed), 14)
    return {
        "images": bell_draw(splits[0], (IMAGES, 3, RES, RES), 1.0, 6.0, ((0, 16), (2, 2))),
        "pos_embed": bell_draw(splits[1], (TOKS, D), 0.5, 3.0, ((0, 2),)),
        "conv_first": bell_draw(splits[2], (3, 3, 3, C1), 13 ** -0.5, 1.75),
        "conv_second": bell_draw(splits[3], (3, 3, C1, C2), (4 * C1) ** -0.5, 0.375),
        "conv_third": bell_draw(splits[4], (3, 3, C2, C3), (4 * C2) ** -0.5, 0.25),
        "conv_fourth": bell_draw(splits[5], (3, 3, C3, C4), (4 * C3) ** -0.5, 0.1875),
        "proj_weight": bell_draw(splits[6], (C4, D), (C4 // 2) ** -0.5, 0.375),
        "ln_first": jnp.clip(1.0 + 0.15 * jax.random.normal(splits[7], (D,), jnp.float32), 0.25, 1.75),
        "qkv_weight": draw_qkv_weight(jax.random.fold_in(splits[13], 71), 0),
        "out_weight": bell_draw(splits[9], (D, D), D ** -0.5, 0.15625, ((0, 2), (1, 16))),
        "ln_second": jnp.clip(1.0 + 0.15 * jax.random.normal(splits[10], (D,), jnp.float32), 0.25, 1.75),
        "up_weight": bell_draw(splits[11], (D, FF), D ** -0.5, 0.15625, ((0, 16), (1, 2))),
        "down_weight": bell_draw(splits[12], (FF, D), (FF // 2) ** -0.5, 0.125, ((0, 2), (1, 16))),
    }


def conv_layer(image_field, kernel, spec):
    out = lax.conv_general_dilated(image_field, kernel, (2, 2), ((1, 1), (1, 1)), dimension_numbers=spec, preferred_element_type=jnp.float32)
    return jax.nn.relu(out).astype(jnp.bfloat16)

def layer_norm(values, gain):
    wide = values.astype(jnp.float32)
    center = wide - lax.optimization_barrier(jnp.mean(wide, axis=-1, keepdims=True))
    spread = lax.optimization_barrier(jnp.mean(center * center, axis=-1, keepdims=True))
    return (center * lax.rsqrt(spread + 1e-06) * gain.astype(jnp.float32)).astype(jnp.bfloat16)

def softmax_mix(query, keys, values):
    head_size = query.shape[-1]
    scores = jnp.einsum('qhd,khd->hqk', query.astype(jnp.float32), keys.astype(jnp.float32)) / jnp.sqrt(jnp.float32(head_size))
    weights = jax.nn.softmax(scores, axis=-1).astype(jnp.bfloat16)
    return jnp.einsum('hqk,khd->qhd', weights.astype(jnp.float32), values.astype(jnp.float32)).astype(jnp.bfloat16)

def block_sum(left, right):
    inner = left.shape[1] // N_SPACE
    left_blocks = left.reshape(left.shape[0], N_SPACE, inner).astype(jnp.float32)
    right_blocks = right.reshape(N_SPACE, inner, right.shape[1]).astype(jnp.float32)
    parts = jnp.einsum('tsk,skd->std', left_blocks, right_blocks).astype(jnp.bfloat16)
    parts = lax.optimization_barrier(parts)
    return lax.optimization_barrier(jnp.sum(parts.astype(jnp.float32), axis=0))

def reference(images, pos_embed, conv_first, conv_second, conv_third, conv_fourth, proj_weight, ln_first, qkv_weight, out_weight, ln_second, up_weight, down_weight):

    def one_image(picture):
        stem_out = conv_layer(picture[None], conv_first, ('NCHW', 'HWIO', 'NHWC'))
        for kernel in (conv_second, conv_third, conv_fourth):
            stem_out = conv_layer(stem_out, kernel, ('NHWC', 'HWIO', 'NHWC'))
        flat = stem_out.reshape(TOKS, C4)
        tokens = (jnp.dot(flat, proj_weight, preferred_element_type=jnp.float32) + pos_embed.astype(jnp.float32)).astype(jnp.bfloat16)
        normed = layer_norm(tokens, ln_first)
        qkv = jnp.dot(normed, qkv_weight.reshape(D, 3 * D), preferred_element_type=jnp.float32).astype(jnp.bfloat16)
        qkv = qkv.reshape(TOKS, 3, HEADS, D // HEADS)
        mixed = softmax_mix(qkv[:, 0], qkv[:, 1], qkv[:, 2]).reshape(TOKS, D)
        after_attn = (tokens.astype(jnp.float32) + block_sum(mixed, out_weight)).astype(jnp.bfloat16)
        normed_two = layer_norm(after_attn, ln_second)
        hidden = jax.nn.gelu(jnp.dot(normed_two, up_weight, preferred_element_type=jnp.float32), approximate=False).astype(jnp.bfloat16)
        encoded = after_attn.astype(jnp.float32) + block_sum(hidden, down_weight)
        return encoded.astype(jnp.bfloat16)
    return lax.map(one_image, images)
```

```python
import functools
import math

import jax
import jax.numpy as jnp
from jax import lax
from jax.experimental import pallas as pl
from jax.experimental.pallas import tpu as pltpu
from jax.sharding import PartitionSpec as P

HEADS = 16
PHASES = 5


def passed_along(value, axis, steps):
    count = lax.axis_size(axis)
    leading, last = (max(0, -steps), min(count, count - steps))
    return lax.ppermute(value, axis, [(source, source + steps) for source in range(leading, last)])


def shifted(value, axis, steps):
    count = lax.axis_size(axis)
    return lax.ppermute(value, axis, [(source, (source + steps) % count) for source in range(count)])


def largest_divisor(number, limit):
    return max(d for d in range(1, limit + 1) if number % d == 0)


def first_conv_body(unroll, field_ref, kernel_ref, out_ref):
    depth = field_ref.shape[1]
    lanes = field_ref.shape[2]

    def step(index, carry):
        for part in range(unroll):
            row = index * unroll + part
            patch = field_ref[pl.ds(2 * row, 3)].reshape(3 * depth, lanes)
            out = lax.dot_general(
                patch, kernel_ref[...], (((0,), (0,)), ((), ())), preferred_element_type=jnp.float32
            )
            out_ref[row] = jnp.maximum(out, 0.0).astype(out_ref.dtype)
        return carry

    lax.fori_loop(0, out_ref.shape[0] // unroll, step, 0)


def first_conv(images, margin, kernel):
    wide = images.shape[3]
    pairs = wide // 4
    channels = images.shape[1]
    out_channels = kernel.shape[3]
    source = lax.broadcasted_iota(jnp.int32, (wide, PHASES, pairs), 0)
    phase = lax.broadcasted_iota(jnp.int32, (wide, PHASES, pairs), 1)
    pair = lax.broadcasted_iota(jnp.int32, (wide, PHASES, pairs), 2)
    pick = (source == 4 * pair + phase - 1).astype(jnp.bfloat16)
    field = jnp.concatenate([margin, images], axis=2)[0]
    rows = field.shape[1]
    picked = jnp.einsum("chw,wqp->hcqp", field, pick, preferred_element_type=jnp.float32)
    picked = picked.astype(jnp.bfloat16).reshape(rows, channels * PHASES, pairs)
    depth = -(-channels * PHASES // 16) * 16
    picked = jnp.pad(picked, ((0, 0), (0, depth - channels * PHASES), (0, 0)))
    taps = jnp.transpose(kernel, (0, 2, 1, 3))
    left = jnp.pad(taps, ((0, 0), (0, 0), (0, 2), (0, 0)))
    right = jnp.pad(taps, ((0, 0), (0, 0), (2, 0), (0, 0)))
    both = jnp.concatenate([left, right], axis=3).reshape(3, channels * PHASES, 2 * out_channels)
    both = jnp.pad(both, ((0, 0), (0, depth - channels * PHASES), (0, 0)))
    both = both.reshape(3 * depth, 2 * out_channels)
    count = (rows - 3) // 2 + 1
    out = pl.pallas_call(
        functools.partial(first_conv_body, largest_divisor(count, 16)),
        out_shape=jax.ShapeDtypeStruct((count, pairs, 2 * out_channels), jnp.bfloat16),
        in_specs=[pl.BlockSpec(memory_space=pltpu.VMEM)] * 2,
        out_specs=pl.BlockSpec(memory_space=pltpu.VMEM),
        compiler_params=pltpu.CompilerParams(vmem_limit_bytes=40 * 1024 * 1024),
        cost_estimate=pl.CostEstimate(
            flops=count * pairs * depth * 3 * 4 * out_channels * 4,
            bytes_accessed=count * pairs * out_channels * 4,
            transcendentals=0,
        ),
    )(picked, both)
    return out[None]


def second_conv(field, kernel):
    height, _, inner, outer = kernel.shape
    before = jnp.concatenate([jnp.zeros_like(kernel[:, 0]), kernel[:, 0]], axis=1)
    here = jnp.concatenate([kernel[:, 1], kernel[:, 2]], axis=1)
    paired = jnp.stack([before, here], axis=1)
    out = lax.conv_general_dilated(
        field,
        paired,
        (2, 1),
        ((0, 0), (1, 0)),
        dimension_numbers=("NHWC", "HWIO", "NHWC"),
        preferred_element_type=jnp.float32,
    )
    return jax.nn.relu(out).astype(jnp.bfloat16)


def later_conv(field, kernel):
    out = lax.conv_general_dilated(
        field,
        kernel,
        (2, 2),
        ((0, 0), (1, 1)),
        dimension_numbers=("NHWC", "HWIO", "NHWC"),
        preferred_element_type=jnp.float32,
    )
    return jax.nn.relu(out).astype(jnp.bfloat16)


def layer_norm(values, gain):
    wide = values.astype(jnp.float32)
    center = wide - jnp.mean(wide, axis=-1, keepdims=True)
    spread = jnp.mean(center * center, axis=-1, keepdims=True)
    return (center * lax.rsqrt(spread + 1e-06) * gain).astype(jnp.bfloat16)


def attend_body(chunks, factor, *refs):
    query_ref, out_ref = refs[0], refs[-1]
    keys, values = refs[1 : 1 + chunks], refs[1 + chunks : 1 + 2 * chunks]
    total = query_ref.shape[1]
    block = largest_divisor(total // 128, 2) * 128
    for start in range(0, total, block):
        query = query_ref[:, start : start + block]
        scores = [
            lax.dot_general(
                key[...], query, (((0,), (0,)), ((), ())), preferred_element_type=jnp.float32
            )
            for key in keys
        ]
        top = functools.reduce(
            jnp.maximum, [jnp.max(score, axis=0, keepdims=True) for score in scores]
        )
        weights = [jnp.exp2((score - top) * factor) for score in scores]
        below = sum(jnp.sum(weight, axis=0, keepdims=True) for weight in weights)
        mixed = sum(
            jnp.dot(value[...], weight.astype(jnp.bfloat16), preferred_element_type=jnp.float32)
            for value, weight in zip(values, weights)
        )
        out_ref[:, start : start + block] = (mixed / below).astype(out_ref.dtype)


def attend(query, keys, values, head_size):
    local, total = query.shape
    chunks = len(keys)
    seen = sum(key.shape[1] for key in keys)
    spec = lambda array: pl.BlockSpec((head_size, array.shape[1]), lambda head: (head, 0))
    factor = math.log2(math.e) / math.sqrt(head_size)
    return pl.pallas_call(
        functools.partial(attend_body, chunks, factor),
        grid=(local // head_size,),
        out_shape=jax.ShapeDtypeStruct((local, total), jnp.bfloat16),
        in_specs=[spec(array) for array in (query, *keys, *values)],
        out_specs=spec(query),
        compiler_params=pltpu.CompilerParams(vmem_limit_bytes=40 * 1024 * 1024),
        cost_estimate=pl.CostEstimate(
            flops=local * total * seen * 16,
            bytes_accessed=local * (2 * total + 2 * seen) * 2,
            transcendentals=(local // head_size) * total * seen,
        ),
    )(query, *keys, *values)


def gathered(weight, axis):
    return lax.all_gather(weight, "dp", axis=axis, tiled=True)


def on_device(
    images,
    pos_embed,
    conv_first,
    conv_second,
    conv_third,
    conv_fourth,
    proj_weight,
    ln_first,
    qkv_weight,
    out_weight,
    ln_second,
    up_weight,
    down_weight,
):
    count = lax.axis_size("space")
    qkv_part = gathered(qkv_weight, 0)
    out_part = gathered(out_weight, 1)
    up_part = gathered(up_weight, 0)
    down_part = gathered(down_weight, 1)
    margin = passed_along(images[:, :, -15:, :], "space", 1)
    positions = [pos_embed] + [shifted(pos_embed, "space", k) for k in range(1, count)]

    stem_out = second_conv(first_conv(images, margin, conv_first), conv_second)
    for kernel in (conv_third, conv_fourth):
        stem_out = later_conv(stem_out, kernel)
    flat = stem_out.reshape(-1, stem_out.shape[3])
    flats = [flat] + [shifted(flat, "space", k) for k in range(1, count)]
    width = proj_weight.shape[1]
    local = qkv_part.shape[2]
    head_size = width // HEADS

    tokens = None
    projected = []
    for rows, position in zip(flats, positions):
        chunk = (
            jnp.dot(rows, proj_weight, preferred_element_type=jnp.float32)
            + position.astype(jnp.float32)
        ).astype(jnp.bfloat16)
        tokens = chunk if tokens is None else tokens
        normed = layer_norm(chunk, ln_first)
        projected.append(
            [
                lax.dot_general(
                    qkv_part[:, which],
                    normed,
                    (((0,), (1,)), ((), ())),
                    preferred_element_type=jnp.float32,
                ).astype(jnp.bfloat16)
                for which in range(3)
            ]
        )
    keys = [part[1] for part in projected]
    values = [part[2] for part in projected]

    def attention_share(query):
        mixed = attend(query, keys, values, head_size)
        share = lax.dot_general(
            mixed, out_part, (((0,), (0,)), ((), ())), preferred_element_type=jnp.float32
        ).astype(jnp.bfloat16)
        return mixed, share

    returned = []
    last = None
    for k in list(range(1, count)) + [0]:
        query = projected[k][0]
        if last is not None:
            query, _ = lax.optimization_barrier((query, last))
        last, share = attention_share(query)
        returned.append(shifted(share, "space", -k) if k else share)
    attn_sum = sum(part.astype(jnp.float32) for part in returned)
    after_attn = (tokens.astype(jnp.float32) + attn_sum).astype(jnp.bfloat16)
    normed_two = layer_norm(after_attn, ln_second)

    def feed_forward(rows):
        before = jnp.dot(rows, up_part, preferred_element_type=jnp.float32)
        hidden = jax.nn.gelu(before, approximate=False).astype(jnp.bfloat16)
        hidden = lax.optimization_barrier(hidden)
        return jnp.dot(hidden, down_part, preferred_element_type=jnp.float32).astype(jnp.bfloat16)

    rows = normed_two.shape[0]
    half = rows // 2
    pieces = [normed_two[:half], normed_two[half:]]
    moved = [[shifted(piece, "space", k) for piece in pieces] for k in range(1, count)]
    totals = feed_forward(normed_two).astype(jnp.float32)
    back = [
        jnp.concatenate([shifted(feed_forward(piece), "space", -k) for piece in there], axis=0)
        for k, there in zip(range(1, count), moved)
    ]
    for part in back:
        totals = totals + part.astype(jnp.float32)
    return (after_attn.astype(jnp.float32) + totals).astype(jnp.bfloat16)[None]


def solution(mesh):
    placed = (
        P("dp", None, "space", None),
        P("space", None),
        P(),
        P(),
        P(),
        P(),
        P(),
        P(),
        P("dp", None, "space"),
        P("space", "dp"),
        P(),
        P("dp", "space"),
        P("space", "dp"),
    )
    return jax.shard_map(
        on_device, mesh=mesh, in_specs=placed, out_specs=P("dp", "space", None), check_vma=False
    )
```

```python
import functools
import math

import jax
import jax.numpy as jnp
from jax import lax
from jax.experimental import pallas as pl
from jax.experimental.pallas import tpu as pltpu
from jax.sharding import PartitionSpec as P

HEADS = 16
PHASES = 5


def passed_along(value, axis, steps):
    count = lax.axis_size(axis)
    leading, last = (max(0, -steps), min(count, count - steps))
    return lax.ppermute(value, axis, [(source, source + steps) for source in range(leading, last)])


def shifted(value, axis, steps):
    count = lax.axis_size(axis)
    return lax.ppermute(value, axis, [(source, (source + steps) % count) for source in range(count)])


def largest_divisor(number, limit):
    return max(d for d in range(1, limit + 1) if number % d == 0)


def first_conv_body(unroll, field_ref, kernel_ref, out_ref):
    depth = field_ref.shape[1]
    lanes = field_ref.shape[2]

    def step(index, carry):
        for part in range(unroll):
            row = index * unroll + part
            patch = field_ref[pl.ds(2 * row, 3)].reshape(3 * depth, lanes)
            out = lax.dot_general(
                patch, kernel_ref[...], (((0,), (0,)), ((), ())), preferred_element_type=jnp.float32
            )
            out_ref[row] = jnp.maximum(out, 0.0).astype(out_ref.dtype)
        return carry

    lax.fori_loop(0, out_ref.shape[0] // unroll, step, 0)


def first_conv(images, margin, kernel):
    wide = images.shape[3]
    pairs = wide // 4
    channels = images.shape[1]
    out_channels = kernel.shape[3]
    source = lax.broadcasted_iota(jnp.int32, (wide, PHASES, pairs), 0)
    phase = lax.broadcasted_iota(jnp.int32, (wide, PHASES, pairs), 1)
    pair = lax.broadcasted_iota(jnp.int32, (wide, PHASES, pairs), 2)
    pick = (source == 4 * pair + phase - 1).astype(jnp.bfloat16)
    field = jnp.concatenate([margin, images], axis=2)[0]
    rows = field.shape[1]
    picked = jnp.einsum("chw,wqp->hcqp", field, pick, preferred_element_type=jnp.float32)
    picked = picked.astype(jnp.bfloat16).reshape(rows, channels * PHASES, pairs)
    depth = -(-channels * PHASES // 16) * 16
    picked = jnp.pad(picked, ((0, 0), (0, depth - channels * PHASES), (0, 0)))
    taps = jnp.transpose(kernel, (0, 2, 1, 3))
    left = jnp.pad(taps, ((0, 0), (0, 0), (0, 2), (0, 0)))
    right = jnp.pad(taps, ((0, 0), (0, 0), (2, 0), (0, 0)))
    both = jnp.concatenate([left, right], axis=3).reshape(3, channels * PHASES, 2 * out_channels)
    both = jnp.pad(both, ((0, 0), (0, depth - channels * PHASES), (0, 0)))
    both = both.reshape(3 * depth, 2 * out_channels)
    count = (rows - 3) // 2 + 1
    out = pl.pallas_call(
        functools.partial(first_conv_body, largest_divisor(count, 16)),
        out_shape=jax.ShapeDtypeStruct((count, pairs, 2 * out_channels), jnp.bfloat16),
        in_specs=[pl.BlockSpec(memory_space=pltpu.VMEM)] * 2,
        out_specs=pl.BlockSpec(memory_space=pltpu.VMEM),
        compiler_params=pltpu.CompilerParams(vmem_limit_bytes=40 * 1024 * 1024),
        cost_estimate=pl.CostEstimate(
            flops=count * pairs * depth * 3 * 4 * out_channels * 4,
            bytes_accessed=count * pairs * out_channels * 4,
            transcendentals=0,
        ),
    )(picked, both)
    return out[None]


def second_conv(field, kernel):
    height, _, inner, outer = kernel.shape
    before = jnp.concatenate([jnp.zeros_like(kernel[:, 0]), kernel[:, 0]], axis=1)
    here = jnp.concatenate([kernel[:, 1], kernel[:, 2]], axis=1)
    paired = jnp.stack([before, here], axis=1)
    out = lax.conv_general_dilated(
        field,
        paired,
        (2, 1),
        ((0, 0), (1, 0)),
        dimension_numbers=("NHWC", "HWIO", "NHWC"),
        preferred_element_type=jnp.float32,
    )
    return jax.nn.relu(out).astype(jnp.bfloat16)


def later_conv(field, kernel):
    out = lax.conv_general_dilated(
        field,
        kernel,
        (2, 2),
        ((0, 0), (1, 1)),
        dimension_numbers=("NHWC", "HWIO", "NHWC"),
        preferred_element_type=jnp.float32,
    )
    return jax.nn.relu(out).astype(jnp.bfloat16)


def layer_norm(values, gain):
    wide = values.astype(jnp.float32)
    center = wide - jnp.mean(wide, axis=-1, keepdims=True)
    spread = jnp.mean(center * center, axis=-1, keepdims=True)
    return (center * lax.rsqrt(spread + 1e-06) * gain).astype(jnp.bfloat16)


def attend_body(chunks, factor, *refs):
    query_ref, out_ref = refs[0], refs[-1]
    keys, values = refs[1 : 1 + chunks], refs[1 + chunks : 1 + 2 * chunks]
    total = query_ref.shape[1]
    block = largest_divisor(total // 128, 2) * 128
    for start in range(0, total, block):
        query = query_ref[:, start : start + block]
        scores = [
            lax.dot_general(
                key[...], query, (((0,), (0,)), ((), ())), preferred_element_type=jnp.float32
            )
            for key in keys
        ]
        top = functools.reduce(
            jnp.maximum, [jnp.max(score, axis=0, keepdims=True) for score in scores]
        )
        weights = [jnp.exp2((score - top) * factor) for score in scores]
        below = sum(jnp.sum(weight, axis=0, keepdims=True) for weight in weights)
        mixed = sum(
            jnp.dot(value[...], weight.astype(jnp.bfloat16), preferred_element_type=jnp.float32)
            for value, weight in zip(values, weights)
        )
        out_ref[:, start : start + block] = (mixed / below).astype(out_ref.dtype)


def attend(query, keys, values, head_size):
    local, total = query.shape
    chunks = len(keys)
    seen = sum(key.shape[1] for key in keys)
    spec = lambda array: pl.BlockSpec((head_size, array.shape[1]), lambda head: (head, 0))
    factor = math.log2(math.e) / math.sqrt(head_size)
    return pl.pallas_call(
        functools.partial(attend_body, chunks, factor),
        grid=(local // head_size,),
        out_shape=jax.ShapeDtypeStruct((local, total), jnp.bfloat16),
        in_specs=[spec(array) for array in (query, *keys, *values)],
        out_specs=spec(query),
        compiler_params=pltpu.CompilerParams(vmem_limit_bytes=40 * 1024 * 1024),
        cost_estimate=pl.CostEstimate(
            flops=local * total * seen * 16,
            bytes_accessed=local * (2 * total + 2 * seen) * 2,
            transcendentals=(local // head_size) * total * seen,
        ),
    )(query, *keys, *values)


def gathered(weight, axis):
    return lax.all_gather(weight, "dp", axis=axis, tiled=True)


def on_device(
    images,
    pos_embed,
    conv_first,
    conv_second,
    conv_third,
    conv_fourth,
    proj_weight,
    ln_first,
    qkv_weight,
    out_weight,
    ln_second,
    up_weight,
    down_weight,
):
    count = lax.axis_size("space")
    attention_part = gathered(
        jnp.concatenate([jnp.moveaxis(qkv_weight, 1, 0), out_weight.T[None]], axis=0), 1
    )
    feed_part = gathered(jnp.stack([up_weight, down_weight.T]), 1)
    out_part = attention_part[3]
    up_part, down_part = feed_part[0], feed_part[1]
    margin = passed_along(images[:, :, -15:, :], "space", 1)
    positions = [pos_embed] + [shifted(pos_embed, "space", k) for k in range(1, count)]

    stem_out = second_conv(first_conv(images, margin, conv_first), conv_second)
    for kernel in (conv_third, conv_fourth):
        stem_out = later_conv(stem_out, kernel)
    flat = stem_out.reshape(-1, stem_out.shape[3])
    flats = [flat] + [shifted(flat, "space", k) for k in range(1, count)]
    width = proj_weight.shape[1]
    local = attention_part.shape[2]
    head_size = width // HEADS

    tokens = None
    projected = []
    for rows, position in zip(flats, positions):
        chunk = (
            jnp.dot(rows, proj_weight, preferred_element_type=jnp.float32)
            + position.astype(jnp.float32)
        ).astype(jnp.bfloat16)
        tokens = chunk if tokens is None else tokens
        normed = layer_norm(chunk, ln_first)
        projected.append(
            [
                lax.dot_general(
                    attention_part[which],
                    normed,
                    (((0,), (1,)), ((), ())),
                    preferred_element_type=jnp.float32,
                ).astype(jnp.bfloat16)
                for which in range(3)
            ]
        )
    keys = [part[1] for part in projected]
    values = [part[2] for part in projected]

    def attention_share(query):
        mixed = attend(query, keys, values, head_size)
        share = lax.dot_general(
            mixed, out_part, (((0,), (1,)), ((), ())), preferred_element_type=jnp.float32
        ).astype(jnp.bfloat16)
        return mixed, share

    returned = []
    last = None
    for k in list(range(1, count)) + [0]:
        query = projected[k][0]
        if last is not None:
            query, _ = lax.optimization_barrier((query, last))
        last, share = attention_share(query)
        returned.append(shifted(share, "space", -k) if k else share)
    attn_sum = sum(part.astype(jnp.float32) for part in returned)
    after_attn = (tokens.astype(jnp.float32) + attn_sum).astype(jnp.bfloat16)
    normed_two = layer_norm(after_attn, ln_second)

    def feed_forward(rows):
        before = jnp.dot(rows, up_part, preferred_element_type=jnp.float32)
        hidden = (0.5 * before * (1.0 + lax.erf(before * math.sqrt(0.5)))).astype(jnp.bfloat16)
        hidden = lax.optimization_barrier(hidden)
        return lax.dot_general(
            hidden, down_part, (((1,), (1,)), ((), ())), preferred_element_type=jnp.float32
        ).astype(jnp.bfloat16)

    rows = normed_two.shape[0]
    half = rows // 2
    pieces = [normed_two[:half], normed_two[half:]]
    moved = [[shifted(piece, "space", k) for piece in pieces] for k in range(1, count)]
    totals = feed_forward(normed_two).astype(jnp.float32)
    back = [
        jnp.concatenate([shifted(feed_forward(piece), "space", -k) for piece in there], axis=0)
        for k, there in zip(range(1, count), moved)
    ]
    for part in back:
        totals = totals + part.astype(jnp.float32)
    return (after_attn.astype(jnp.float32) + totals).astype(jnp.bfloat16)[None]


def solution(mesh):
    placed = (
        P("dp", None, "space", None),
        P("space", None),
        P(),
        P(),
        P(),
        P(),
        P(),
        P(),
        P("dp", None, "space"),
        P("space", "dp"),
        P(),
        P("dp", "space"),
        P("space", "dp"),
    )
    return jax.shard_map(
        on_device, mesh=mesh, in_specs=placed, out_specs=P("dp", "space", None), check_vma=False
    )
```
